32 devices in a mesh: row: 8 (over z, core), col: 4 (over y, x).
Axes of the slice: x: 2, y: 2, z: 4, core: 2. Of those that a mesh axis runs over, the one named last changes fastest.
Arguments:
- gradient: float32 [8192, 28672], P('row', 'col'), may hold values from -100 to 100
- residual: float32 [8192, 28672], P('row', 'col'), may hold values from -3 to 3
- q_init: float32 [4, 28672], P(None, 'col'), may hold values from -5 to 5
Outputs:
- q_factor: float32 [4, 28672], P(None, 'col')
- new_residual: float32 [8192, 28672], P('row', 'col')
The draws below stay inside these ranges and needn't reach their ends.
All inputs are finite; a program needn't handle non-finite values.
Results may differ from the reference program's by a relative error of at most 0.00012.
Values sent between devices are 32-bit elements; how exact they have to be, the bound alone decides.
A program may use at most 128 MiB of HBM per device.

```python
import jax
import jax.numpy as jnp
from jax import lax

D = 8192
FF = 28672
RANK = 4
ITERS = 16


def draw_gradient(key, part):
    key_rows = jax.random.fold_in(key, 11)
    key_cols = jax.random.fold_in(key, 12)
    key_noise = jax.random.fold_in(key, 13)
    row_index = jnp.arange(D).astype(jnp.float32)
    rising = jnp.exp(jnp.log(3.0) * row_index / D)
    row_scale = rising * jnp.exp(jax.random.uniform(key_rows, (D,), jnp.float32, 0.0, jnp.log(10.0))) / 4.0
    col_scale = jnp.exp(jax.random.uniform(key_cols, (FF,), jnp.float32, 0.0, jnp.log(10.0))) / 3.0
    noise_draw = jnp.clip(jax.random.normal(key_noise, (D, FF), jnp.float32), -4.0, 4.0)
    return (noise_draw * row_scale[:, None] * col_scale[None, :]).astype(jnp.float32)


def block_scale(key, extent, shards, least, high):
    factor_of = 1.0
    for position, parts in shards:
        heights = jax.random.uniform(jax.random.fold_in(jax.random.fold_in(key, 6), position), (parts,), jnp.float32, least / len(shards), high / len(shards))
        factor_of = factor_of * jnp.repeat(jnp.exp(heights), extent[position] // parts).reshape((-1,) + (1,) * (len(extent) - 1 - position))
    return factor_of


def centred(stream_key, extent, scale, most, split=(), kind=jnp.bfloat16):
    entries = jax.random.normal(stream_key, extent, jnp.float32) * scale
    if len(split) > 0:
        entries = block_scale(stream_key, extent, split, -0.22, 0.18) * entries
    return jnp.clip(entries, min=-most, max=most).astype(kind)


def setup_inputs(seed: int = 0) -> dict:
    seeds = jax.random.split(jax.random.key(seed), 4)
    gradient = draw_gradient(jax.random.fold_in(seeds[3], 71), 0)
    residual = centred(seeds[1], (D, FF), 0.5, 3.0, ((0, 8), (1, 4)), jnp.float32)
    q_init = centred(seeds[2], (RANK, FF), 1.0, 5.0, ((1, 4),), jnp.float32)
    return dict(gradient=gradient, residual=residual, q_init=q_init)


def reference(gradient, residual, q_init):
    highest = lax.Precision.HIGHEST
    merged = gradient + residual

    def iterate(step_index, carry):
        q_current, p_previous = carry
        p_factor = lax.dot_general(q_current.astype(jnp.float32), merged.astype(jnp.float32), (((1,), (1,)), ((), ())), precision=highest, preferred_element_type=jnp.float32)
        gram = lax.dot_general(p_factor.astype(jnp.float32), p_factor.astype(jnp.float32), (((1,), (1,)), ((), ())), precision=highest, preferred_element_type=jnp.float32)
        factor_low = jnp.linalg.cholesky(gram)
        p_basis = jax.scipy.linalg.solve_triangular(factor_low, p_factor, lower=True)
        q_next = jnp.dot(p_basis.astype(jnp.float32), merged.astype(jnp.float32), precision=highest, preferred_element_type=jnp.float32)
        return (q_next, p_basis)
    start = (q_init, jnp.zeros((RANK, D), jnp.float32))
    q_factor, p_basis = lax.fori_loop(0, ITERS, iterate, start)
    approx = lax.dot_general(p_basis.astype(jnp.float32), q_factor.astype(jnp.float32), (((0,), (0,)), ((), ())), precision=highest, preferred_element_type=jnp.float32)
    return (q_factor, merged - approx)
```

```python
import functools

import jax
import jax.numpy as jnp
from jax import lax
from jax.experimental import pallas as pl
from jax.experimental.pallas import tpu as pltpu
from jax.sharding import PartitionSpec as P

ITERS = 16
MESH = pl.DeviceIdType.MESH
LANE = 128
SUB = 8


def factor(gram):
    low = [[None] * 4 for _ in range(4)]
    for i in range(4):
        for j in range(i + 1):
            rest = gram[i][j]
            for k in range(j):
                rest = rest - low[i][k] * low[j][k]
            low[i][j] = jnp.sqrt(rest) if i == j else rest / low[j][j]
    return low


def solve(low, rows):
    found = []
    for i in range(4):
        rest = rows[i]
        for k in range(i):
            rest = rest - low[i][k] * found[k]
        found.append(rest / low[i][i])
    return found


def kernel(
    n_row, n_col, chunks,
    grad_ref, res_ref, q0_ref, q_out, p_out,
    m, slot, acc, pb, qb, p_mine, p_in, p_sum, c_mine, c_in, q_all,
    g_sem, r_sem, a_send, a_recv, b_send, b_recv, c_send, c_recv,
):
    rows, cols = m.shape
    width = q_all.shape[-1]
    tiles = width // LANE
    groups = cols // width
    chunk = rows // chunks
    me_row, me_col = lax.axis_index("row"), lax.axis_index("col")
    col_peer = lambda d: (me_row, lax.rem(me_col + d, n_col))
    row_peer = lambda d: (lax.rem(me_row + d, n_row), me_col)

    barrier = pltpu.get_barrier_semaphore()
    for d in range(1, n_col):
        pl.semaphore_signal(barrier, inc=1, device_id=col_peer(d), device_id_type=MESH)
    for d in range(1, n_row):
        pl.semaphore_signal(barrier, inc=1, device_id=row_peer(d), device_id_type=MESH)

    def grad_copy(i):
        part = pl.ds(i * chunk, chunk)
        return pltpu.make_async_copy(grad_ref.at[part], m.at[part], g_sem.at[i])

    def res_copy(i):
        part = pl.ds(i * chunk, chunk)
        return pltpu.make_async_copy(res_ref.at[part], slot.at[i % 2], r_sem.at[i % 2])

    for i in range(chunks):
        grad_copy(i).start()
        if i < 2:
            res_copy(i).start()
    for g in range(groups):
        part = slice(g * width, (g + 1) * width)
        q_now = q0_ref[:, part]
        for r in range(4):
            qb[r, :, part] = jnp.broadcast_to(q_now[r : r + 1], (SUB, width))
    c_mine[...] = jnp.zeros_like(c_mine)
    for i in range(chunks):
        grad_copy(i).wait()
        res_copy(i).wait()

        @pl.loop(0, chunk // SUB)
        def _(k):
            here = pl.ds(pl.multiple_of(i * chunk + k * SUB, SUB), SUB)
            m[here, :] += slot[i % 2, pl.ds(pl.multiple_of(k * SUB, SUB), SUB), :]

        if i + 2 < chunks:
            res_copy(i + 2).start()
    pl.semaphore_wait(barrier, n_col + n_row - 2)

    high = 32

    def iterate(step, carry):
        par = lax.rem(step, 2)

        @pl.loop(0, rows // high)
        def _(k):
            here = pl.ds(pl.multiple_of(k * high, high), high)
            totals = [jnp.zeros((high // SUB, SUB, LANE), jnp.float32)] * 4
            for c in range(cols // LANE):
                part = slice(c * LANE, (c + 1) * LANE)
                piece = m[here, part].reshape(high // SUB, SUB, LANE)
                for r in range(4):
                    totals[r] = totals[r] + piece * qb[r, :, part][None]
            for r in range(4):
                acc[r, here, :] = totals[r].reshape(high, LANE)

        for b in range(rows // LANE):
            part = slice(b * LANE, (b + 1) * LANE)
            sums = [jnp.sum(acc[r, part, :].T, axis=0, keepdims=True) for r in range(4)]
            p_mine[0, :, part] = jnp.concatenate(sums, axis=0)

        def p_copy(d):
            return pltpu.make_async_remote_copy(
                src_ref=p_mine.at[0], dst_ref=p_in.at[par, d],
                send_sem=a_send.at[d], recv_sem=a_recv.at[par, d],
                device_id=col_peer(d), device_id_type=MESH,
            )

        for d in range(1, n_col):
            p_copy(d).start()
        for d in range(1, n_col):
            p_copy(d).wait()
        p_now = p_mine[0]
        for d in range(1, n_col):
            p_now = p_now + p_in[par, d]
        p_sum[0] = p_now

        row_id = lax.broadcasted_iota(jnp.int32, (4, LANE), 0)
        lane_id = lax.broadcasted_iota(jnp.int32, (4, LANE), 1)
        corner = jnp.zeros((4, LANE), jnp.float32)
        for i in range(4):
            dots = jnp.sum(p_now * p_now[i : i + 1], axis=1, keepdims=True)
            corner = jnp.where(lane_id == i, dots, corner)
        for s in range(n_row):
            c_mine[s, :, width:] = corner
        for r in range(4):
            for b in range(rows // LANE):
                part = slice(b * LANE, (b + 1) * LANE)
                pb[r, part, :] = jnp.broadcast_to(p_now[r : r + 1, part], (LANE, LANE)).T

        @pl.loop(0, groups)
        def _(g):
            def add(k, totals):
                totals = list(totals)
                for u in range(high // SUB):
                    here = pl.ds(pl.multiple_of(k * high + u * SUB, SUB), SUB)
                    scale = [pb[r, here, :] for r in range(4)]
                    for t in range(tiles):
                        piece = m[here, pl.ds(pl.multiple_of(g * width + t * LANE, LANE), LANE)]
                        for r in range(4):
                            totals[r * tiles + t] = totals[r * tiles + t] + piece * scale[r]
                return tuple(totals)

            start = (jnp.zeros((SUB, LANE), jnp.float32),) * (4 * tiles)
            totals = lax.fori_loop(0, rows // high, add, start)
            for t in range(tiles):
                sums = [
                    jnp.sum(totals[r * tiles + t], axis=0, keepdims=True) for r in range(4)
                ]
                c_mine[g, :, t * LANE : (t + 1) * LANE] = jnp.concatenate(sums, axis=0)

        def c_copy(d):
            return pltpu.make_async_remote_copy(
                src_ref=c_mine.at[lax.rem(me_row + d, n_row)], dst_ref=c_in.at[par, d],
                send_sem=b_send.at[d], recv_sem=b_recv.at[par, d],
                device_id=row_peer(d), device_id_type=MESH,
            )

        for d in range(1, n_row):
            c_copy(d).start()
        for d in range(1, n_row):
            c_copy(d).wait()
        cross = c_mine[me_row]
        for d in range(1, n_row):
            cross = cross + c_in[par, d]
        gram = [
            [cross[i : i + 1, width + j : width + j + 1] for j in range(4)] for i in range(4)
        ]
        low = factor(gram)
        q_rows = solve(low, [cross[r : r + 1, :width] for r in range(4)])
        q_all[par, me_row] = jnp.concatenate(q_rows, axis=0)

        def q_copy(d):
            mine = q_all.at[par, me_row]
            return pltpu.make_async_remote_copy(
                src_ref=mine, dst_ref=mine,
                send_sem=c_send.at[d], recv_sem=c_recv.at[par, d],
                device_id=row_peer(d), device_id_type=MESH,
            )

        for d in range(1, n_row):
            q_copy(d).start()
        p_held = p_sum[0]
        p_rows = solve(low, [p_held[r : r + 1] for r in range(4)])
        p_out[...] = jnp.concatenate(p_rows + p_rows, axis=0)
        for d in range(1, n_row):
            q_copy(d).wait()
        for g in range(groups):
            q_now = q_all[par, g]
            for r in range(4):
                qb[r, :, g * width : (g + 1) * width] = jnp.broadcast_to(
                    q_now[r : r + 1], (SUB, width)
                )
        return carry

    lax.fori_loop(0, ITERS, iterate, 0)
    for g in range(groups):
        q_now = q_all[(ITERS - 1) % 2, g]
        q_out[:, g * width : (g + 1) * width] = jnp.concatenate([q_now, q_now], axis=0)


def shards(n_row, n_col, gradient, residual, q_init):
    rows, cols = gradient.shape
    width = -(-cols // (LANE * n_row)) * LANE
    chunks = 8
    f32 = jnp.float32
    vmem = lambda *shape: pltpu.VMEM(shape, f32)
    dma = pltpu.SemaphoreType.DMA
    q_wide, p_basis = pl.pallas_call(
        functools.partial(kernel, n_row, n_col, chunks),
        out_shape=(
            jax.ShapeDtypeStruct((SUB, cols), f32),
            jax.ShapeDtypeStruct((SUB, rows), f32),
        ),
        in_specs=[
            pl.BlockSpec(memory_space=pl.ANY),
            pl.BlockSpec(memory_space=pl.ANY),
            pl.BlockSpec(memory_space=pltpu.VMEM),
        ],
        out_specs=(
            pl.BlockSpec(memory_space=pltpu.VMEM),
            pl.BlockSpec(memory_space=pltpu.VMEM),
        ),
        scratch_shapes=[
            vmem(rows, cols),
            vmem(2, rows // chunks, cols),
            vmem(4, rows, LANE),
            vmem(4, rows, LANE),
            vmem(4, SUB, cols),
            vmem(3, 4, rows),
            vmem(3, n_col, 4, rows),
            vmem(3, 4, rows),
            vmem(n_row + 2, 4, width + LANE),
            vmem(3, n_row, 4, width + LANE),
            vmem(3, n_row, 4, width),
            dma((chunks,)),
            dma((2,)),
            dma((n_col,)),
            dma((2, n_col)),
            dma((n_row,)),
            dma((2, n_row)),
            dma((n_row,)),
            dma((2, n_row)),
        ],
        compiler_params=pltpu.CompilerParams(
            collective_id=0, has_side_effects=True, vmem_limit_bytes=60 * 1024 * 1024
        ),
    )(gradient, residual, jnp.pad(q_init, ((0, SUB - 4), (0, 0))))
    q_factor = q_wide[:4]
    left = gradient + residual
    for r in range(4):
        left = left - p_basis[r][:, None] * q_factor[r][None, :]
    return (q_factor, left)


def solution(mesh):
    in_specs = (P("row", "col"), P("row", "col"), P(None, "col"))
    out_specs = (P(None, "col"), P("row", "col"))
    body = functools.partial(shards, mesh.shape["row"], mesh.shape["col"])
    return jax.shard_map(body, mesh=mesh, in_specs=in_specs, out_specs=out_specs, check_vma=False)
```
